32 devices in a mesh: dp: 4 (over y, x), expert: 4 (over z), tensor: 2 (over core).
Axes of the slice: x: 2, y: 2, z: 4, core: 2. Of those that a mesh axis runs over, the one named last changes fastest.
Arguments:
- tokens: bfloat16 [2048, 2560], P(('dp', 'expert')), may hold values from -6 to 6
- norm_gain: float32 [2560], replicated, may hold values from 0.5 to 1.5
- expert_ids: int32 [2048, 6], P(('dp', 'expert')), may hold values from 0 to 31, all different within a row; in each aligned block of 128 rows (0 to 127, 128 to 255, ...) at most 48 rows name the same one
- route_weights: int32 [2048, 6], P(('dp', 'expert')), may hold values from 1 to 64
- w_gate: bfloat16 [32, 2560, 768], P('expert', None, 'tensor'), may hold values from -0.125 to 0.125
- w_up: bfloat16 [32, 2560, 768], P('expert', None, 'tensor'), may hold values from -0.125 to 0.125
- w_down: bfloat16 [32, 768, 2560], P('expert', 'tensor'), may hold values from -0.21875 to 0.21875
- shared_gate: bfloat16 [2560, 2048], P(None, ('dp', 'tensor')), may hold values from -0.125 to 0.125
- shared_up: bfloat16 [2560, 2048], P(None, ('dp', 'tensor')), may hold values from -0.125 to 0.125
- shared_down: bfloat16 [2048, 2560], P(('dp', 'tensor')), may hold values from -0.125 to 0.125
Outputs:
- mixed: bfloat16 [2048, 2560], P(('dp', 'expert'), 'tensor')
The draws below stay inside these ranges and needn't reach their ends.
Inputs may be any that keep to these rules, and one draw needn't show every extreme that they name: `expert_ids`: each row names 6 different experts. In each aligned block of 128 rows (the rows of one index of dp+expert) no expert is named by more than 48 rows, a bound that some blocks reach.
All inputs are finite; a program needn't handle non-finite values.
Results may differ from the reference program's by a relative error of at most 0.011.
Values may be sent and summed in bfloat16 or wider, within the bound.
A program may use at most 128 MiB of HBM per device.

```python
import math
import jax
import jax.numpy as jnp
import numpy as np
from jax import lax

D = 2560
FF = 768
SFF = 2048
EXPERTS = 32
TOP = 6
TOK_DEV = 128
CAP = 48
TOKENS = 2048


def place_ends(values, own_key, low, largest):
    spot = [jax.random.randint(jax.random.fold_in(own_key, axis), (), 0, length) for axis, length in enumerate(values.shape)]
    widest = values.shape.index(max(values.shape))
    next_to = spot[:widest] + [(spot[widest] + 1) % values.shape[widest]] + spot[widest + 1:]
    return values.at[tuple(spot)].set(low).at[tuple(next_to)].set(largest)


def shard_levels(rng, extent, split, low, largest):
    loudness = 1.0
    for dim, parts in split:
        draws = jax.random.uniform(jax.random.fold_in(jax.random.fold_in(rng, 6), dim), (parts,), jnp.float32, low / len(split), largest / len(split))
        loudness = loudness * jnp.repeat(jnp.exp(draws), extent[dim] // parts).reshape((-1,) + (1,) * (len(extent) - 1 - dim))
    return loudness


def deal_out(key, own, number, rows, number_of, top, reach, slope):
    ranking = jax.random.permutation(key, number_of)
    crowded, usual = portions_of(number_of, rows * top, reach, slope, True), portions_of(number_of, rows * top, reach, slope, False)
    places = jnp.arange(number_of)

    def named(tallies, offset_by):
        used = int((tallies > 0).sum())
        fixed = max(1, used // 4)
        shifted = fixed + (places - fixed + offset_by * (used - fixed)) % max(1, number_of - fixed)
        return jnp.zeros((number_of,), jnp.int32).at[ranking[jnp.where(places < fixed, places, shifted)]].set(jnp.asarray(tallies, jnp.int32))

    tallies = jnp.where(number % 4 == 0, named(crowded, number // 4), named(usual, number - number // 4 - 1))
    mixed = jax.random.permutation(jax.random.fold_in(own, 3), number_of)
    donor, taker = mixed[0:number_of // 2 * 2:2], mixed[1:number_of // 2 * 2:2]
    slack = jnp.minimum(tallies[donor] - 1, reach - tallies[taker]) // 2
    slack = jnp.where((donor == ranking[0]) | (taker == ranking[0]) | (tallies[taker] == 0), 0, jnp.maximum(slack, 0))
    shifted = jax.random.randint(jax.random.fold_in(own, 4), (number_of // 2,), 0, 1 << 20) % (slack + 1)
    tallies = tallies.at[donor].add(-shifted).at[taker].add(shifted)
    labels = jnp.searchsorted(jnp.cumsum(tallies), jnp.arange(rows * top), side="right").astype(jnp.int32)
    table = labels.reshape(top, rows).T
    table = table[jax.random.permutation(jax.random.fold_in(own, 1), rows)]
    offset_by = jax.random.randint(jax.random.fold_in(own, 2), (rows, 1), 0, top)
    return jnp.take_along_axis(table, (jnp.arange(top)[None, :] + offset_by) % top, axis=1)


def portions_of(count, total, limit, skew, full):
    portions = [(1 << 20) // math.isqrt(standing ** skew) + 1 for standing in range(1, count + 1)]
    largest = limit if full else min(limit, max(-(-total // count), total * portions[0] // sum(portions)))
    least = 1 if total - largest >= count - 1 else 0
    holding, rest = [largest] + [least] * (count - 1), total - largest - least * (count - 1)
    while rest > 0:
        movable = [i for i in range(1, count) if holding[i] < largest] or [i for i in range(1, count) if holding[i] < limit]
        pool, left = sum([portions[i] for i in movable]), rest
        for i in movable:
            extra = min(limit - holding[i], max(1, left * portions[i] // pool), rest)
            holding[i] = holding[i] + extra
            rest = rest - extra
    return np.array(holding)


def bell_draw(rng, dims, deviation, bound, cuts=(), kind=jnp.bfloat16):
    values = jax.random.normal(rng, dims, jnp.float32) * deviation
    if len(cuts) > 0:
        values = shard_levels(rng, dims, cuts, -0.22, 0.18) * values
    return jnp.clip(values, min=-bound, max=bound).astype(kind)


def setup_inputs(seed: int = 0) -> dict:
    keys = jax.random.split(jax.random.key(seed), 11)
    tokens = bell_draw(keys[0], (TOKENS, D), 1.0, 6.0, ((0, 16),))
    norm_gain = jnp.clip(1.0 + 0.1 * jax.random.normal(keys[1], (D,), jnp.float32), 0.5, 1.5)
    expert_ids_keys = jax.random.split(jax.random.fold_in(keys[2], 1), TOKENS // TOK_DEV)
    expert_ids_turns = jax.random.permutation(jax.random.fold_in(keys[2], 3), TOKENS // TOK_DEV)
    expert_ids = jax.vmap(lambda own, number: deal_out(jax.random.fold_in(keys[2], 2), own, number, TOK_DEV, EXPERTS, TOP, CAP, 2))(expert_ids_keys, expert_ids_turns).reshape((TOKENS, TOP))
    route_weights = place_ends(jax.random.randint(keys[3], (TOKENS, TOP), 1, 65), jax.random.fold_in(keys[3], 1), 1, 64).astype(jnp.int32)
    w_gate = bell_draw(keys[4], (EXPERTS, D, FF), D ** -0.5, 0.125, ((0, 4), (2, 2)))
    w_up = bell_draw(keys[5], (EXPERTS, D, FF), D ** -0.5, 0.125, ((0, 4), (2, 2)))
    w_down = bell_draw(keys[6], (EXPERTS, FF, D), FF ** -0.5, 0.21875, ((0, 4), (1, 2)))
    shared_gate = bell_draw(keys[7], (D, SFF), D ** -0.5, 0.125, ((1, 8),))
    shared_up = bell_draw(keys[8], (D, SFF), D ** -0.5, 0.125, ((1, 8),))
    shared_down = bell_draw(keys[9], (SFF, D), SFF ** -0.5, 0.125, ((0, 8),))
    return {"tokens": tokens, "norm_gain": norm_gain, "expert_ids": expert_ids, "route_weights": route_weights, "w_gate": w_gate, "w_up": w_up, "w_down": w_down, "shared_gate": shared_gate, "shared_up": shared_up, "shared_down": shared_down}


EPSILON = 1e-06

def normalize(tokens, norm_gain):
    values = tokens.astype(jnp.float32)
    inverse = lax.rsqrt(lax.optimization_barrier(jnp.mean(values * values, axis=1, keepdims=True)) + EPSILON)
    return (values * inverse * norm_gain.astype(jnp.float32)[None, :]).astype(jnp.bfloat16)

def reference(tokens, norm_gain, expert_ids, route_weights, w_gate, w_up, w_down, shared_gate, shared_up, shared_down):
    normed = normalize(tokens, norm_gain)
    groups = TOKENS // TOK_DEV
    pair_total = TOK_DEV * TOP
    local_ids = expert_ids.reshape(groups, pair_total).astype(jnp.int32)
    onehot = (local_ids[:, :, None] == jnp.arange(EXPERTS, dtype=jnp.int32)[None, None, :]).astype(jnp.int32)
    earlier = jnp.cumsum(onehot, axis=1) - onehot
    slot_index = lax.optimization_barrier(jnp.sum(earlier * onehot, axis=2)).astype(jnp.int32)
    position = (local_ids * CAP + slot_index).astype(jnp.int32)
    group_index = jnp.broadcast_to(jnp.arange(groups, dtype=jnp.int32)[:, None], (groups, pair_total)).astype(jnp.int32)
    pair_token = (group_index * TOK_DEV + jnp.arange(pair_total, dtype=jnp.int32)[None, :] // TOP).astype(jnp.int32)
    filler = jnp.full((groups, EXPERTS * CAP), -1, jnp.int32).at[group_index, position].set(pair_token)
    pair_scale = route_weights.astype(jnp.float32).reshape(groups, pair_total) / 64.0
    slot_scale = jnp.zeros((groups, EXPERTS * CAP), jnp.float32).at[group_index, position].set(pair_scale)
    filler = filler.reshape(groups, EXPERTS, CAP).transpose(1, 0, 2).reshape(EXPERTS, groups * CAP)
    slot_scale = slot_scale.reshape(groups, EXPERTS, CAP).transpose(1, 0, 2).reshape(EXPERTS, groups * CAP)

    def expert_step(totals, inputs):
        owner_rows, owner_scale, gate_weight, up_weight, down_weight = inputs
        valid = owner_rows >= 0
        safe_rows = jnp.maximum(owner_rows, 0).astype(jnp.int32)
        picked = jnp.where(valid[:, None], normed[safe_rows], jnp.zeros((), jnp.bfloat16))
        gate_value = jnp.dot(picked, gate_weight, preferred_element_type=jnp.float32)
        up_value = jnp.dot(picked, up_weight, preferred_element_type=jnp.float32)
        hidden = (jax.nn.silu(gate_value) * up_value).astype(jnp.bfloat16)
        result = jnp.dot(hidden, down_weight, preferred_element_type=jnp.float32).astype(jnp.bfloat16)
        update = result.astype(jnp.float32) * owner_scale[:, None]
        update = jnp.where(valid[:, None], update, jnp.zeros((), jnp.float32))
        return (totals.at[safe_rows].add(update), None)
    routed, unused = lax.scan(expert_step, jnp.zeros((TOKENS, D), jnp.float32), (filler, slot_scale, w_gate, w_up, w_down))
    shared_gate_value = jnp.dot(normed, shared_gate, preferred_element_type=jnp.float32)
    shared_up_value = jnp.dot(normed, shared_up, preferred_element_type=jnp.float32)
    shared_hidden = (jax.nn.silu(shared_gate_value) * shared_up_value).astype(jnp.bfloat16)
    shared_out = jnp.dot(shared_hidden, shared_down, preferred_element_type=jnp.float32)
    return (shared_out + routed).astype(jnp.bfloat16)
```

```python
import jax
import jax.numpy as jnp
from jax import lax
from jax.sharding import PartitionSpec as P

EPSILON = 1e-06
LANES = 128


def normalize(tokens, norm_gain):
    values = tokens.astype(jnp.float32)
    inverse = lax.rsqrt(jnp.mean(values * values, axis=1, keepdims=True) + EPSILON)
    return (values * inverse * norm_gain[None, :]).astype(jnp.bfloat16)


def by_owner(partial, blocks, width):
    rows = partial.shape[0] // blocks
    parts = partial.shape[1] // width
    split = partial.reshape(blocks, rows, parts, width)
    return split.transpose(0, 2, 1, 3).reshape(blocks * parts * rows, width)


def on_device(
    tokens,
    norm_gain,
    expert_ids,
    route_weights,
    w_gate,
    w_up,
    w_down,
    shared_gate,
    shared_up,
    shared_down,
):
    normed = normalize(tokens, norm_gain)
    rows, width = normed.shape
    owners = lax.axis_size("expert")
    groups = lax.axis_size("dp")
    half = width // lax.axis_size("tensor")
    local = w_gate.shape[0]
    experts = local * owners
    lanes = -(-experts // LANES) * LANES
    match = expert_ids[:, :, None] == jnp.arange(lanes, dtype=jnp.int32)[None, None, :]
    scale = jnp.sum(jnp.where(match, route_weights[:, :, None], 0), axis=1)
    scale = (scale.astype(jnp.float32) / 64.0).astype(jnp.bfloat16)
    sent = jnp.concatenate([normed, scale], axis=1)
    everyone = lax.all_gather(sent, "expert", axis=0, tiled=True)
    routed_rows = everyone[:, :width]
    first = lax.axis_index("expert") * local
    mine = lax.dynamic_slice_in_dim(everyone[:, width:], first, local, 1).astype(jnp.float32)
    hidden = []
    for e in range(local):
        gate = jnp.dot(routed_rows, w_gate[e], preferred_element_type=jnp.float32)
        up = jnp.dot(routed_rows, w_up[e], preferred_element_type=jnp.float32)
        hidden.append((jax.nn.silu(gate) * up * mine[:, e : e + 1]).astype(jnp.bfloat16))
    hidden = jnp.concatenate(hidden, axis=1)
    routed = jnp.dot(hidden, w_down.reshape(-1, width), preferred_element_type=jnp.float32)
    routed = by_owner(routed.astype(jnp.bfloat16), owners, half)
    routed = lax.psum_scatter(routed, ("expert", "tensor"), scatter_dimension=0, tiled=True)

    piece = lax.all_gather(normed, "dp", axis=0, tiled=True)
    gate = jnp.dot(piece, shared_gate, preferred_element_type=jnp.float32)
    up = jnp.dot(piece, shared_up, preferred_element_type=jnp.float32)
    shared = (jax.nn.silu(gate) * up).astype(jnp.bfloat16)
    shared = jnp.dot(shared, shared_down, preferred_element_type=jnp.float32)
    shared = by_owner(shared.astype(jnp.bfloat16), groups, half)
    shared = lax.psum_scatter(shared, ("dp", "tensor"), scatter_dimension=0, tiled=True)
    return (shared.astype(jnp.float32) + routed.astype(jnp.float32)).astype(jnp.bfloat16)


def solution(mesh):
    placed = (
        P(("dp", "expert"), None),
        P(),
        P(("dp", "expert"), None),
        P(("dp", "expert"), None),
        P("expert", None, "tensor"),
        P("expert", None, "tensor"),
        P("expert", "tensor", None),
        P(None, ("dp", "tensor")),
        P(None, ("dp", "tensor")),
        P(("dp", "tensor"), None),
    )
    return jax.shard_map(
        on_device,
        mesh=mesh,
        in_specs=placed,
        out_specs=P(("dp", "expert"), "tensor"),
        check_vma=False,
    )
```

```python
import functools

import jax
import jax.numpy as jnp
from jax import lax
from jax.experimental import pallas as pl
from jax.experimental.pallas import tpu as pltpu
from jax.sharding import PartitionSpec as P

EPSILON = 1e-06
LANES = 128
MESH = pl.DeviceIdType.MESH
VMEM_BYTES = 67043328


def dot(a, b):
    return jnp.dot(a, b, preferred_element_type=jnp.float32)


def kernel(
    owners,
    groups,
    tokens,
    gain,
    ids,
    weights,
    w_gate,
    w_up,
    w_down,
    shared_gate,
    shared_up,
    shared_down,
    out,
    blocks,
    peers,
    gate_up,
    down,
    shared_in,
    shared_out,
    hidden,
    shared_hidden,
    staged,
    keep,
    total,
    partner_routed,
    partner_shared,
    landed,
    load_sem,
    shared_sem,
    token_sem,
    zsend,
    zrecv,
    gsend,
    grecv,
    fsend,
    frecv,
    esend,
    erecv,
    rsend,
    rrecv,
):
    g = lax.axis_index("dp")
    z = lax.axis_index("expert")
    c = lax.axis_index("tensor")
    other = 1 - c
    local, ff, width = w_down.shape
    sff = shared_down.shape[0]
    rows = tokens.shape[0]
    half = width // 2
    lanes = blocks.shape[2] - width
    my_rows = pl.ds(pl.multiple_of(c * (rows // 2), rows // 2), rows // 2)
    its_rows = pl.ds(pl.multiple_of(other * (rows // 2), rows // 2), rows // 2)

    token_loads = [
        pltpu.make_async_copy(tokens.at[:, pl.ds(p * half, half)], staged.at[p], token_sem.at[p])
        for p in range(2)
    ]
    for load in token_loads:
        load.start()

    def expert_loads(e):
        first = pl.ds(pl.multiple_of(e * ff, LANES), ff)
        return (
            pltpu.make_async_copy(w_gate.at[e], gate_up.at[e, :, pl.ds(0, ff)], load_sem.at[0, e]),
            pltpu.make_async_copy(w_up.at[e], gate_up.at[e, :, pl.ds(ff, ff)], load_sem.at[1, e]),
            pltpu.make_async_copy(w_down.at[e], down.at[first], load_sem.at[2, e]),
        )

    shared_loads = (
        pltpu.make_async_copy(shared_gate, shared_in.at[:, pl.ds(0, sff)], shared_sem.at[0]),
        pltpu.make_async_copy(shared_up, shared_in.at[:, pl.ds(sff, sff)], shared_sem.at[1]),
        pltpu.make_async_copy(shared_down, shared_out, shared_sem.at[2]),
    )
    for e in range(local):
        expert_loads(e)[0].start()
        expert_loads(e)[1].start()
    for e in range(local):
        expert_loads(e)[2].start()
    for load in shared_loads:
        load.start()

    barrier = pltpu.get_barrier_semaphore()
    for r in range(1, owners):
        peer = {"expert": lax.rem(z + r, owners)}
        pl.semaphore_signal(barrier, inc=1, device_id=peer, device_id_type=MESH)
    for r in range(1, groups):
        peer = {"dp": lax.rem(g + r, groups)}
        pl.semaphore_signal(barrier, inc=1, device_id=peer, device_id_type=MESH)
    pl.semaphore_signal(barrier, inc=1, device_id={"tensor": other}, device_id_type=MESH)

    for load in token_loads:
        load.wait()
    step = 16

    def norm(t, carry):
        span = pl.ds(pl.multiple_of(t * step, step), step)
        left = staged[0, span, :].astype(jnp.float32)
        right = staged[1, span, :].astype(jnp.float32)
        square = jnp.sum(left * left, axis=1, keepdims=True)
        square = square + jnp.sum(right * right, axis=1, keepdims=True)
        inverse = lax.rsqrt(square / width + EPSILON)
        blocks[z, span, 0:half] = (left * inverse * gain[:, 0:half]).astype(jnp.bfloat16)
        blocks[z, span, half:width] = (right * inverse * gain[:, half:width]).astype(jnp.bfloat16)
        lane = lax.broadcasted_iota(jnp.int32, (step, lanes), 1)
        scale = jnp.zeros((step, lanes), jnp.float32)
        for k in range(ids.shape[1]):
            weight = weights[span, k : k + 1].astype(jnp.float32) / 64.0
            scale = scale + jnp.where(ids[span, k : k + 1] == lane, weight, 0.0)
        blocks[z, span, width : width + lanes] = scale.astype(jnp.bfloat16)
        return carry

    lax.fori_loop(0, rows // step, norm, 0)

    pl.semaphore_wait(barrier, owners + groups - 1)

    def block_send(r):
        return pltpu.make_async_remote_copy(
            src_ref=blocks.at[z, my_rows],
            dst_ref=blocks.at[z, my_rows],
            send_sem=zsend.at[r - 1],
            recv_sem=zrecv.at[z],
            device_id={"expert": lax.rem(z + r, owners)},
            device_id_type=MESH,
        )

    def peer_send(r):
        return pltpu.make_async_remote_copy(
            src_ref=blocks.at[z, my_rows, pl.ds(0, width)],
            dst_ref=peers.at[r - 1, my_rows],
            send_sem=gsend.at[r - 1],
            recv_sem=grecv.at[r - 1],
            device_id={"dp": lax.rem(g + r, groups)},
            device_id_type=MESH,
        )

    for r in sorted(range(1, owners), key=lambda r: min(r, owners - r)):
        block_send(r).start()
    for r in range(1, groups):
        peer_send(r).start()

    def pass_on(ref, span, index):
        return pltpu.make_async_remote_copy(
            src_ref=ref.at[span],
            dst_ref=ref.at[span],
            send_sem=fsend.at[index],
            recv_sem=frecv.at[index],
            device_id={"tensor": other},
            device_id_type=MESH,
        )

    def exchange(slot, where, index):
        return pltpu.make_async_remote_copy(
            src_ref=staged.at[slot],
            dst_ref=where,
            send_sem=esend.at[index],
            recv_sem=erecv.at[index],
            device_id={"tensor": other},
            device_id_type=MESH,
        )

    def result_send(src, slot, device):
        return pltpu.make_async_remote_copy(
            src_ref=src,
            dst_ref=landed.at[slot],
            send_sem=rsend.at[slot],
            recv_sem=rrecv.at[slot],
            device_id=device,
            device_id_type=MESH,
        )

    upper = z >= owners // 2
    near = jnp.where(upper, owners - 1 - z, z)

    def source(i):
        walk = jnp.where(i > near, i, near - i)
        return jnp.where(upper, owners - 1 - walk, walk)

    def fetch(i):
        b = source(i)
        pltpu.make_async_copy(blocks.at[b, my_rows], blocks.at[b, my_rows], zrecv.at[b]).wait()
        pass_on(blocks.at[b], my_rows, b).start()

    chunk = 256
    spans = half // chunk

    def routed(i, own):
        b = source(i)
        if not own:
            pass_on(blocks.at[b], its_rows, b).wait_recv()
        first = z * local

        def expert(e, carry):
            if own:
                expert_loads(e)[0].wait()
                expert_loads(e)[1].wait()
            both = dot(blocks[b, :, 0:width], gate_up[e])
            gate = both[:, 0:ff]
            lane = lax.broadcasted_iota(jnp.int32, (rows, lanes), 1)
            scale = blocks[b, :, width : width + lanes].astype(jnp.float32)
            scale = jnp.sum(jnp.where(lane == first + e, scale, 0.0), axis=1, keepdims=True)
            value = gate / (1.0 + jnp.exp(-gate)) * both[:, ff:] * scale
            hidden[:, pl.ds(pl.multiple_of(e * ff, LANES), ff)] = value.astype(jnp.bfloat16)
            return carry

        lax.fori_loop(0, local, expert, 0)
        if own:
            fetch(1)
            for e in range(local):
                expert_loads(e)[2].wait()
        else:

            @pl.when(i + 1 < owners)
            def _():
                fetch(i + 1)

        def theirs(n, carry):
            at = pl.ds(pl.multiple_of(other * half + n * chunk, LANES), chunk)
            to = pl.ds(pl.multiple_of(n * chunk, LANES), chunk)
            staged[0, :, to] = dot(hidden[...], down[:, at]).astype(jnp.bfloat16)
            return carry

        def ours(n, carry):
            at = pl.ds(pl.multiple_of(c * half + n * chunk, LANES), chunk)
            to = pl.ds(pl.multiple_of(n * chunk, LANES), chunk)
            keep[:, to] = dot(hidden[...], down[:, at])
            return carry

        lax.fori_loop(0, spans, theirs, 0)
        swap = exchange(0, partner_routed.at[i], i)
        swap.start()
        lax.fori_loop(0, spans, ours, 0)
        swap.wait()
        if own:
            total[...] = keep[...] + partner_routed[i].astype(jnp.float32)
        else:
            summed = keep[...] + partner_routed[i].astype(jnp.float32)
            partner_routed[i] = summed.astype(jnp.bfloat16)
            slot = lax.rem(z - b + owners, owners) - 1
            result_send(partner_routed.at[i], slot, {"expert": b}).start()

    def shared_first(j, block):
        both = dot(block, shared_in[...])
        gate = both[:, 0:sff]
        value = gate / (1.0 + jnp.exp(-gate)) * both[:, sff:]
        shared_hidden[j] = value.astype(jnp.bfloat16)

    routed(0, True)

    for r in range(1, groups):
        here = peers.at[r - 1, my_rows]
        pltpu.make_async_copy(here, here, grecv.at[r - 1]).wait()
        pass_on(peers.at[r - 1], my_rows, owners + r - 1).start()
    for load in shared_loads:
        load.wait()
    shared_first(0, blocks[z, :, 0:width])

    def shared_peer(j, carry):
        pass_on(peers.at[j - 1], its_rows, owners + j - 1).wait_recv()
        shared_first(j, peers[j - 1])
        return carry

    lax.fori_loop(1, groups, shared_peer, 0)

    def shared_theirs(j, carry):
        at = pl.ds(pl.multiple_of(other * half, LANES), half)
        staged[j] = dot(shared_hidden[j], shared_out[:, at]).astype(jnp.bfloat16)
        exchange(j, partner_shared.at[j], owners + j).start()
        return carry

    lax.fori_loop(0, groups, shared_theirs, 0)

    def shared_ours(j, carry):
        at = pl.ds(pl.multiple_of(c * half, LANES), half)
        keep[...] = dot(shared_hidden[j], shared_out[:, at])
        exchange(j, partner_shared.at[j], owners + j).wait()
        summed = keep[...] + partner_shared[j].astype(jnp.float32)

        @pl.when(j == 0)
        def _():
            total[...] = total[...] + summed

        @pl.when(j > 0)
        def _():
            partner_shared[j] = summed.astype(jnp.bfloat16)
            device = {"dp": lax.rem(g - j + groups, groups)}
            result_send(partner_shared.at[j], owners - 1 + j - 1, device).start()

        return carry

    lax.fori_loop(0, groups, shared_ours, 0)

    def others(i, carry):
        routed(i, False)
        return carry

    lax.fori_loop(1, owners, others, 0)

    for s in range(owners + groups - 2):
        result_send(partner_routed.at[0], s, {"tensor": other}).wait_recv()
    final = total[...]
    for s in range(owners + groups - 2):
        final = final + landed[s].astype(jnp.float32)
    staged[0] = final.astype(jnp.bfloat16)
    store = pltpu.make_async_copy(staged.at[0], out, token_sem.at[0])
    store.start()
    for r in range(1, owners):
        block_send(r).wait_send()
        b = lax.rem(z + r, owners)
        pass_on(blocks.at[b], my_rows, b).wait_send()
    for r in range(1, groups):
        peer_send(r).wait_send()
        pass_on(peers.at[r - 1], my_rows, owners + r - 1).wait_send()
    for s in range(owners + groups - 2):
        result_send(partner_routed.at[0], s, {"tensor": other}).wait_send()
    store.wait()


def on_device(owners, groups, tokens, norm_gain, expert_ids, route_weights, *matrices):
    w_gate, w_up, w_down, shared_gate, shared_up, shared_down = matrices
    rows, width = tokens.shape
    half = width // 2
    local, ff, _ = w_down.shape
    sff = shared_down.shape[0]
    lanes = -(-local * owners // LANES) * LANES
    bf16, f32 = jnp.bfloat16, jnp.float32
    dma = pltpu.SemaphoreType.DMA
    vmem = pl.BlockSpec(memory_space=pltpu.VMEM)
    anywhere = pl.BlockSpec(memory_space=pl.ANY)
    links = owners + groups
    return pl.pallas_call(
        functools.partial(kernel, owners, groups),
        out_shape=jax.ShapeDtypeStruct((rows, half), bf16),
        in_specs=[anywhere, vmem, vmem, vmem] + [anywhere] * 6,
        out_specs=anywhere,
        scratch_shapes=[
            pltpu.VMEM((owners, rows, width + lanes), bf16),
            pltpu.VMEM((groups - 1, rows, width), bf16),
            pltpu.VMEM((local, width, 2 * ff), bf16),
            pltpu.VMEM((local * ff, width), bf16),
            pltpu.VMEM((width, 2 * sff), bf16),
            pltpu.VMEM((sff, width), bf16),
            pltpu.VMEM((rows, local * ff), bf16),
            pltpu.VMEM((groups, rows, sff), bf16),
            pltpu.VMEM((max(groups, 2), rows, half), bf16),
            pltpu.VMEM((rows, half), f32),
            pltpu.VMEM((rows, half), f32),
            pltpu.VMEM((owners, rows, half), bf16),
            pltpu.VMEM((groups, rows, half), bf16),
            pltpu.VMEM((links - 2, rows, half), bf16),
            dma((3, local)),
            dma((3,)),
            dma((2,)),
            dma((owners - 1,)),
            dma((owners,)),
            dma((groups - 1,)),
            dma((groups - 1,)),
            dma((links - 1,)),
            dma((links - 1,)),
            dma((links,)),
            dma((links,)),
            dma((links - 2,)),
            dma((links - 2,)),
        ],
        compiler_params=pltpu.CompilerParams(
            collective_id=0, has_side_effects=True, vmem_limit_bytes=VMEM_BYTES
        ),
    )(tokens, norm_gain[None, :], expert_ids, route_weights, *matrices)


def solution(mesh):
    placed = (
        P(("dp", "expert"), None),
        P(),
        P(("dp", "expert"), None),
        P(("dp", "expert"), None),
        P("expert", None, "tensor"),
        P("expert", None, "tensor"),
        P("expert", "tensor", None),
        P(None, ("dp", "tensor")),
        P(None, ("dp", "tensor")),
        P(("dp", "tensor"), None),
    )
    return jax.shard_map(
        functools.partial(on_device, mesh.shape["expert"], mesh.shape["dp"]),
        mesh=mesh,
        in_specs=placed,
        out_specs=P(("dp", "expert"), "tensor"),
        check_vma=False,
    )
```

```python
import functools

import jax
import jax.numpy as jnp
from jax import lax
from jax.experimental import pallas as pl
from jax.experimental.pallas import tpu as pltpu
from jax.sharding import PartitionSpec as P

EPSILON = 1e-06
LANES = 128
MESH = pl.DeviceIdType.MESH
VMEM_BYTES = 67043328


def dot(a, b):
    return jnp.dot(a, b, preferred_element_type=jnp.float32)


def kernel(
    owners,
    groups,
    tokens,
    gain,
    ids,
    weights,
    w_gate,
    w_up,
    w_down,
    shared_gate,
    shared_up,
    shared_down,
    out,
    blocks,
    peers,
    gate_up,
    down,
    shared_in,
    shared_out,
    hidden,
    shared_hidden,
    staged,
    keep,
    total,
    partner_routed,
    partner_shared,
    landed,
    load_sem,
    shared_sem,
    token_sem,
    zsend,
    zrecv,
    gsend,
    grecv,
    fsend,
    frecv,
    esend,
    erecv,
    rsend,
    rrecv,
):
    g = lax.axis_index("dp")
    z = lax.axis_index("expert")
    c = lax.axis_index("tensor")
    other = 1 - c
    local, ff, width = w_down.shape
    sff = shared_down.shape[0]
    rows = tokens.shape[0]
    half = width // 2
    lanes = blocks.shape[2] - width
    my_rows = pl.ds(pl.multiple_of(c * (rows // 2), rows // 2), rows // 2)
    its_rows = pl.ds(pl.multiple_of(other * (rows // 2), rows // 2), rows // 2)

    token_loads = [
        pltpu.make_async_copy(tokens.at[:, pl.ds(p * half, half)], staged.at[p], token_sem.at[p])
        for p in range(2)
    ]
    for load in token_loads:
        load.start()

    def expert_loads(e):
        first = pl.ds(pl.multiple_of(e * ff, LANES), ff)
        return (
            pltpu.make_async_copy(w_gate.at[e], gate_up.at[e, :, pl.ds(0, ff)], load_sem.at[0, e]),
            pltpu.make_async_copy(w_up.at[e], gate_up.at[e, :, pl.ds(ff, ff)], load_sem.at[1, e]),
            pltpu.make_async_copy(w_down.at[e], down.at[first], load_sem.at[2, e]),
        )

    shared_loads = (
        pltpu.make_async_copy(shared_gate, shared_in.at[:, pl.ds(0, sff)], shared_sem.at[0]),
        pltpu.make_async_copy(shared_up, shared_in.at[:, pl.ds(sff, sff)], shared_sem.at[1]),
        pltpu.make_async_copy(shared_down, shared_out, shared_sem.at[2]),
    )
    for e in range(local):
        expert_loads(e)[0].start()
        expert_loads(e)[1].start()
    for e in range(local):
        expert_loads(e)[2].start()
    for load in shared_loads:
        load.start()

    barrier = pltpu.get_barrier_semaphore()
    for r in range(1, owners):
        peer = {"expert": lax.rem(z + r, owners)}
        pl.semaphore_signal(barrier, inc=1, device_id=peer, device_id_type=MESH)
    for r in range(1, groups):
        peer = {"dp": lax.rem(g + r, groups)}
        pl.semaphore_signal(barrier, inc=1, device_id=peer, device_id_type=MESH)
    pl.semaphore_signal(barrier, inc=1, device_id={"tensor": other}, device_id_type=MESH)

    for load in token_loads:
        load.wait()
    step = 16

    def norm(t, carry):
        span = pl.ds(pl.multiple_of(t * step, step), step)
        left = staged[0, span, :].astype(jnp.float32)
        right = staged[1, span, :].astype(jnp.float32)
        square = jnp.sum(left * left, axis=1, keepdims=True)
        square = square + jnp.sum(right * right, axis=1, keepdims=True)
        inverse = lax.rsqrt(square / width + EPSILON)
        blocks[z, span, 0:half] = (left * inverse * gain[:, 0:half]).astype(jnp.bfloat16)
        blocks[z, span, half:width] = (right * inverse * gain[:, half:width]).astype(jnp.bfloat16)
        lane = lax.broadcasted_iota(jnp.int32, (step, lanes), 1)
        scale = jnp.zeros((step, lanes), jnp.float32)
        for k in range(ids.shape[1]):
            weight = weights[span, k : k + 1].astype(jnp.float32) / 64.0
            scale = scale + jnp.where(ids[span, k : k + 1] == lane, weight, 0.0)
        blocks[z, span, width : width + lanes] = scale.astype(jnp.bfloat16)
        return carry

    lax.fori_loop(0, rows // step, norm, 0)

    pl.semaphore_wait(barrier, owners + groups - 1)

    def block_send(b, way):
        return pltpu.make_async_remote_copy(
            src_ref=blocks.at[b, my_rows],
            dst_ref=blocks.at[b, my_rows],
            send_sem=zsend.at[way, b],
            recv_sem=zrecv.at[b],
            device_id={"expert": lax.rem(z + (1 if way else owners - 1), owners)},
            device_id_type=MESH,
        )

    def peer_send(r):
        return pltpu.make_async_remote_copy(
            src_ref=blocks.at[z, my_rows, pl.ds(0, width)],
            dst_ref=peers.at[r - 1, my_rows],
            send_sem=gsend.at[r - 1],
            recv_sem=grecv.at[r - 1],
            device_id={"dp": lax.rem(g + r, groups)},
            device_id_type=MESH,
        )

    @pl.when(z + 1 < owners)
    def _():
        block_send(z, 1).start()

    @pl.when(z > 0)
    def _():
        block_send(z, 0).start()

    for r in range(1, groups):
        peer_send(r).start()

    def pass_on(ref, span, index):
        return pltpu.make_async_remote_copy(
            src_ref=ref.at[span],
            dst_ref=ref.at[span],
            send_sem=fsend.at[index],
            recv_sem=frecv.at[index],
            device_id={"tensor": other},
            device_id_type=MESH,
        )

    def exchange(slot, where, index):
        return pltpu.make_async_remote_copy(
            src_ref=staged.at[slot],
            dst_ref=where,
            send_sem=esend.at[index],
            recv_sem=erecv.at[index],
            device_id={"tensor": other},
            device_id_type=MESH,
        )

    def result_send(src, slot, device):
        return pltpu.make_async_remote_copy(
            src_ref=src,
            dst_ref=landed.at[slot],
            send_sem=rsend.at[slot],
            recv_sem=rrecv.at[slot],
            device_id=device,
            device_id_type=MESH,
        )

    upper = z >= owners // 2
    near = jnp.where(upper, owners - 1 - z, z)

    def source(i):
        walk = jnp.where(i > near, i, near - i)
        return jnp.where(upper, owners - 1 - walk, walk)

    def arrive(b):
        pltpu.make_async_copy(blocks.at[b, my_rows], blocks.at[b, my_rows], zrecv.at[b]).wait()

    def fetch(d):
        @pl.when(z - d >= 0)
        def _():
            arrive(z - d)

            @pl.when(z + 1 < owners)
            def _():
                block_send(z - d, 1).start()

            pass_on(blocks.at[z - d], my_rows, z - d).start()

        @pl.when(z + d < owners)
        def _():
            arrive(z + d)

            @pl.when(z > 0)
            def _():
                block_send(z + d, 0).start()

            pass_on(blocks.at[z + d], my_rows, z + d).start()

    chunk = 256
    spans = half // chunk

    def routed(i, own):
        b = source(i)
        if not own:
            pass_on(blocks.at[b], its_rows, b).wait_recv()
        first = z * local

        def expert(e, carry):
            if own:
                expert_loads(e)[0].wait()
                expert_loads(e)[1].wait()
            both = dot(blocks[b, :, 0:width], gate_up[e])
            gate = both[:, 0:ff]
            lane = lax.broadcasted_iota(jnp.int32, (rows, lanes), 1)
            scale = blocks[b, :, width : width + lanes].astype(jnp.float32)
            scale = jnp.sum(jnp.where(lane == first + e, scale, 0.0), axis=1, keepdims=True)
            value = gate / (1.0 + jnp.exp(-gate)) * both[:, ff:] * scale
            hidden[:, pl.ds(pl.multiple_of(e * ff, LANES), ff)] = value.astype(jnp.bfloat16)
            return carry

        lax.fori_loop(0, local, expert, 0)
        if own:
            fetch(1)
            for e in range(local):
                expert_loads(e)[2].wait()
        else:

            @pl.when(i + 2 < owners)
            def _():
                fetch(i + 2)

        def theirs(n, carry):
            at = pl.ds(pl.multiple_of(other * half + n * chunk, LANES), chunk)
            to = pl.ds(pl.multiple_of(n * chunk, LANES), chunk)
            staged[0, :, to] = dot(hidden[...], down[:, at]).astype(jnp.bfloat16)
            return carry

        def ours(n, carry):
            at = pl.ds(pl.multiple_of(c * half + n * chunk, LANES), chunk)
            to = pl.ds(pl.multiple_of(n * chunk, LANES), chunk)
            keep[:, to] = dot(hidden[...], down[:, at])
            return carry

        lax.fori_loop(0, spans, theirs, 0)
        swap = exchange(0, partner_routed.at[i], i)
        swap.start()
        lax.fori_loop(0, spans, ours, 0)
        swap.wait()
        if own:
            total[...] = keep[...] + partner_routed[i].astype(jnp.float32)
        else:
            summed = keep[...] + partner_routed[i].astype(jnp.float32)
            partner_routed[i] = summed.astype(jnp.bfloat16)
            slot = lax.rem(z - b + owners, owners) - 1
            result_send(partner_routed.at[i], slot, {"expert": b}).start()

    def shared_first(j, block):
        both = dot(block, shared_in[...])
        gate = both[:, 0:sff]
        value = gate / (1.0 + jnp.exp(-gate)) * both[:, sff:]
        shared_hidden[j] = value.astype(jnp.bfloat16)

    routed(0, True)

    for r in range(1, groups):
        here = peers.at[r - 1, my_rows]
        pltpu.make_async_copy(here, here, grecv.at[r - 1]).wait()
        pass_on(peers.at[r - 1], my_rows, owners + r - 1).start()
    for load in shared_loads:
        load.wait()
    shared_first(0, blocks[z, :, 0:width])

    def shared_peer(j, carry):
        pass_on(peers.at[j - 1], its_rows, owners + j - 1).wait_recv()
        shared_first(j, peers[j - 1])
        return carry

    lax.fori_loop(1, groups, shared_peer, 0)

    def shared_theirs(j, carry):
        at = pl.ds(pl.multiple_of(other * half, LANES), half)
        staged[j] = dot(shared_hidden[j], shared_out[:, at]).astype(jnp.bfloat16)
        exchange(j, partner_shared.at[j], owners + j).start()
        return carry

    lax.fori_loop(0, groups, shared_theirs, 0)
    if owners > 2:
        fetch(2)

    def shared_ours(j, carry):
        at = pl.ds(pl.multiple_of(c * half, LANES), half)
        keep[...] = dot(shared_hidden[j], shared_out[:, at])
        exchange(j, partner_shared.at[j], owners + j).wait()
        summed = keep[...] + partner_shared[j].astype(jnp.float32)

        @pl.when(j == 0)
        def _():
            total[...] = total[...] + summed

        @pl.when(j > 0)
        def _():
            partner_shared[j] = summed.astype(jnp.bfloat16)
            device = {"dp": lax.rem(g - j + groups, groups)}
            result_send(partner_shared.at[j], owners - 1 + j - 1, device).start()

        return carry

    lax.fori_loop(0, groups, shared_ours, 0)

    def others(i, carry):
        routed(i, False)
        return carry

    lax.fori_loop(1, owners, others, 0)

    for s in range(owners + groups - 2):
        result_send(partner_routed.at[0], s, {"tensor": other}).wait_recv()
    final = total[...]
    for s in range(owners + groups - 2):
        final = final + landed[s].astype(jnp.float32)
    staged[0] = final.astype(jnp.bfloat16)
    store = pltpu.make_async_copy(staged.at[0], out, token_sem.at[0])
    store.start()
    for r in range(1, owners):
        b = lax.rem(z + r, owners)
        pass_on(blocks.at[b], my_rows, b).wait_send()
    for b in range(owners):

        @pl.when((b <= z) & (z + 1 < owners))
        def _():
            block_send(b, 1).wait_send()

        @pl.when((b >= z) & (z > 0))
        def _():
            block_send(b, 0).wait_send()

    for r in range(1, groups):
        peer_send(r).wait_send()
        pass_on(peers.at[r - 1], my_rows, owners + r - 1).wait_send()
    for s in range(owners + groups - 2):
        result_send(partner_routed.at[0], s, {"tensor": other}).wait_send()
    store.wait()


def on_device(owners, groups, tokens, norm_gain, expert_ids, route_weights, *matrices):
    w_gate, w_up, w_down, shared_gate, shared_up, shared_down = matrices
    rows, width = tokens.shape
    half = width // 2
    local, ff, _ = w_down.shape
    sff = shared_down.shape[0]
    lanes = -(-local * owners // LANES) * LANES
    bf16, f32 = jnp.bfloat16, jnp.float32
    dma = pltpu.SemaphoreType.DMA
    vmem = pl.BlockSpec(memory_space=pltpu.VMEM)
    anywhere = pl.BlockSpec(memory_space=pl.ANY)
    links = owners + groups
    return pl.pallas_call(
        functools.partial(kernel, owners, groups),
        out_shape=jax.ShapeDtypeStruct((rows, half), bf16),
        in_specs=[anywhere, vmem, vmem, vmem] + [anywhere] * 6,
        out_specs=anywhere,
        scratch_shapes=[
            pltpu.VMEM((owners, rows, width + lanes), bf16),
            pltpu.VMEM((groups - 1, rows, width), bf16),
            pltpu.VMEM((local, width, 2 * ff), bf16),
            pltpu.VMEM((local * ff, width), bf16),
            pltpu.VMEM((width, 2 * sff), bf16),
            pltpu.VMEM((sff, width), bf16),
            pltpu.VMEM((rows, local * ff), bf16),
            pltpu.VMEM((groups, rows, sff), bf16),
            pltpu.VMEM((max(groups, 2), rows, half), bf16),
            pltpu.VMEM((rows, half), f32),
            pltpu.VMEM((rows, half), f32),
            pltpu.VMEM((owners, rows, half), bf16),
            pltpu.VMEM((groups, rows, half), bf16),
            pltpu.VMEM((links - 2, rows, half), bf16),
            dma((3, local)),
            dma((3,)),
            dma((2,)),
            dma((2, owners)),
            dma((owners,)),
            dma((groups - 1,)),
            dma((groups - 1,)),
            dma((links - 1,)),
            dma((links - 1,)),
            dma((links,)),
            dma((links,)),
            dma((links - 2,)),
            dma((links - 2,)),
        ],
        compiler_params=pltpu.CompilerParams(
            collective_id=0, has_side_effects=True, vmem_limit_bytes=VMEM_BYTES
        ),
    )(tokens, norm_gain[None, :], expert_ids, route_weights, *matrices)


def solution(mesh):
    placed = (
        P(("dp", "expert"), None),
        P(),
        P(("dp", "expert"), None),
        P(("dp", "expert"), None),
        P("expert", None, "tensor"),
        P("expert", None, "tensor"),
        P("expert", "tensor", None),
        P(None, ("dp", "tensor")),
        P(None, ("dp", "tensor")),
        P(("dp", "tensor"), None),
    )
    return jax.shard_map(
        functools.partial(on_device, mesh.shape["expert"], mesh.shape["dp"]),
        mesh=mesh,
        in_specs=placed,
        out_specs=P(("dp", "expert"), "tensor"),
        check_vma=False,
    )
```
